256 devices in a mesh: row: 16 (over z_lo, x, core), col: 16 (over y, z_hi).
Axes of the slice: x: 4, y: 4, z: 8 (z_hi: 4, z_lo: 2; z = z_hi * 2 + z_lo), core: 2. Of those that a mesh axis runs over, the one named last changes fastest.
Arguments:
- inputs: bfloat16 [2048, 8192], P('col', 'row'), may hold values from -6 to 6
- cotangent: bfloat16 [2048, 8192], P('col', 'row'), may hold values from -6 to 6
- gate_pre: bfloat16 [2048, 16384], P('row', 'col'), may hold values from -8 to 8
- up_pre: bfloat16 [2048, 16384], P('row', 'col'), may hold values from -6 to 6
- w_gate: bfloat16 [8192, 16384], P('row', 'col'), may hold values from -0.0625 to 0.0625
- w_up: bfloat16 [8192, 16384], P('row', 'col'), may hold values from -0.0625 to 0.0625
- w_down: bfloat16 [16384, 8192], P('col', 'row'), may hold values from -0.046875 to 0.046875
Outputs:
- grad_inputs: bfloat16 [2048, 8192], P('col', 'row')
- grad_gate: float32 [8192, 16384], P('row', 'col')
- grad_up: float32 [8192, 16384], P('row', 'col')
- grad_down: float32 [16384, 8192], P('col', 'row')
The draws below stay inside these ranges and needn't reach their ends.
All inputs are finite; a program needn't handle non-finite values.
Results may differ from the reference program's by a relative error of at most 0.0049.
Values may be sent and summed in bfloat16 or wider, within the bound.
No kernel may reach another device: no remote copies, remote signals or barrier semaphores. Data moves between devices by JAX's collectives and lax.ppermute only.
A program may use at most 128 MiB of HBM per device.

```python
import math
import jax
import jax.numpy as jnp

D = 8192
FF = 16384
TOKENS = 2048


def block_scale(own_key, extent, shards, smallest, largest):
    gain = 1.0
    for axis_at, parts in shards:
        draws = jax.random.uniform(jax.random.fold_in(jax.random.fold_in(own_key, 6), axis_at), (parts,), jnp.float32, smallest / len(shards), largest / len(shards))
        gain = gain * jnp.repeat(jnp.exp(draws), extent[axis_at] // parts).reshape((-1,) + (1,) * (len(extent) - 1 - axis_at))
    return gain


def normal_values(own_key, dims, spread, most, cuts=(), kind=jnp.bfloat16):
    level = block_scale(own_key, dims, cuts, -0.22, 0.18) if cuts else 1.0
    entries = jax.random.normal(own_key, dims, jnp.float32) * spread * level
    return jnp.minimum(jnp.maximum(entries, -most), most).astype(kind)


def setup_inputs(seed: int = 0) -> dict:
    splits = jax.random.split(jax.random.key(seed), 8)
    return {
        "inputs": normal_values(splits[0], (TOKENS, D), 1.0, 6.0, ((0, 16), (1, 16))),
        "cotangent": normal_values(splits[1], (TOKENS, D), 1.0, 6.0, ((0, 16), (1, 16))),
        "gate_pre": normal_values(splits[2], (TOKENS, FF), 1.5, 8.0, ((0, 16), (1, 16))),
        "up_pre": normal_values(splits[3], (TOKENS, FF), 1.0, 6.0, ((0, 16), (1, 16))),
        "w_gate": normal_values(splits[4], (D, FF), D ** -0.5, 0.0625, ((0, 16), (1, 16))),
        "w_up": normal_values(splits[5], (D, FF), D ** -0.5, 0.0625, ((0, 16), (1, 16))),
        "w_down": normal_values(splits[6], (FF, D), FF ** -0.5, 0.046875, ((0, 16), (1, 16))),
    }


def reference(inputs, cotangent, gate_pre, up_pre, w_gate, w_up, w_down):
    gate_f = gate_pre.astype(jnp.float32)
    up_f = up_pre.astype(jnp.float32)
    sig = jax.nn.sigmoid(gate_f)
    act = gate_f * sig
    hidden = (act * up_f).astype(jnp.bfloat16)
    grad_hidden = jnp.dot(cotangent, w_down.T, preferred_element_type=jnp.float32)
    grad_gate_pre = (grad_hidden * up_f * sig * (1.0 + gate_f * (1.0 - sig))).astype(jnp.bfloat16)
    grad_up_pre = (grad_hidden * act).astype(jnp.bfloat16)
    grad_inputs = jnp.dot(grad_gate_pre, w_gate.T, preferred_element_type=jnp.float32)
    grad_inputs = grad_inputs + jnp.dot(grad_up_pre, w_up.T, preferred_element_type=jnp.float32)
    scale = 1.0 / math.sqrt(inputs.shape[0])
    grad_gate = jnp.dot(inputs.T, grad_gate_pre, preferred_element_type=jnp.float32) * scale
    grad_up = jnp.dot(inputs.T, grad_up_pre, preferred_element_type=jnp.float32) * scale
    grad_down = jnp.dot(hidden.T, cotangent, preferred_element_type=jnp.float32) * scale
    return (grad_inputs.astype(jnp.bfloat16), grad_gate, grad_up, grad_down)
```

```python
import math

import jax
import jax.numpy as jnp
from jax import lax
from jax.sharding import Mesh
from jax.sharding import PartitionSpec as P


ROW = ("zl", "x", "core")
COL = ("y", "zh")
CHIPS = ("zl", "x")
BF16 = jnp.bfloat16
F32 = jnp.float32


def shift(a, axis, by):
    n = lax.axis_size(axis)
    return lax.ppermute(a, axis, [(i, (i + by) % n) for i in range(n)])


def pick(a, i):
    return lax.dynamic_index_in_dim(a, i, 0, False)


def put(out, a, i, at=0):
    return lax.dynamic_update_slice(out, a[None], (i, at) + (0,) * (a.ndim - 1))


def gather_direct(a, axis):
    n = lax.axis_size(axis)
    i = lax.axis_index(axis)
    out = put(jnp.zeros((n,) + a.shape, a.dtype), a, i)
    for by in (1, n - 1, 2):
        out = put(out, shift(a, axis, by), (i - by) % n)
    return out


def gather_ring(a, axis):
    n = lax.axis_size(axis)
    i = lax.axis_index(axis)
    half = a.shape[0] // 2
    up = shift(a, axis, 1)
    down = shift(a, axis, n - 1)
    far_up = shift(up[:half], axis, 1)
    far_down = shift(down[half:], axis, n - 1)
    out = put(jnp.zeros((n,) + a.shape, a.dtype), a, i)
    out = put(out, up, (i - 1) % n)
    out = put(out, down, (i + 1) % n)
    out = put(out, far_up, (i + 2) % n)
    return put(out, far_down, (i + 2) % n, half)


def gather_col(a):
    rows, n = a.shape
    z = gather_direct(a, "zh")
    out = gather_ring(z.reshape(4 * rows, n), "y")
    return out.reshape(16 * rows, n)


def gather_chips(a):
    zl = lax.axis_index("zl")
    both = put(put(jnp.zeros((2,) + a.shape, a.dtype), a, zl), shift(a, "zl", 1), 1 - zl)
    out = gather_ring(both.reshape((-1,) + a.shape[1:]), "x")
    out = out.reshape((4, 2) + a.shape)
    return out.swapaxes(0, 1)


def exchange_sum(blocks, axis):
    got = lax.all_to_all(blocks, axis, 0, 0, tiled=True)
    return got.astype(F32).sum(0)


def exchange_sum_permute(blocks, axis):
    n = lax.axis_size(axis)
    i = lax.axis_index(axis)
    total = pick(blocks, i).astype(F32)
    for by in (1, n - 1, 2):
        total = total + shift(pick(blocks, (i + by) % n), axis, by).astype(F32)
    return total


def swiglu_back(gate_pre, up_pre, grad_hidden):
    gate_f = gate_pre.astype(F32)
    up_f = up_pre.astype(F32)
    grad_hidden = grad_hidden.astype(F32)
    sig = jax.nn.sigmoid(gate_f)
    act = gate_f * sig
    hidden = (act * up_f).astype(BF16)
    grad_gate_pre = (grad_hidden * up_f * sig * (1.0 + gate_f * (1.0 - sig))).astype(BF16)
    grad_up_pre = (grad_hidden * act).astype(BF16)
    return (hidden, grad_gate_pre, grad_up_pre)


def contract_last(left, right):
    return lax.dot_general(left, right, (((1,), (1,)), ((), ())), preferred_element_type=F32)


def contract_first(left, right):
    return lax.dot_general(left, right, (((0,), (0,)), ((), ())), preferred_element_type=F32)


def per_device(inputs, cotangent, gate_pre, up_pre, w_gate, w_up, w_down):
    core = lax.axis_index("core")
    rows = inputs.shape[0]
    half = rows // 2
    dim = inputs.shape[1]
    ff = gate_pre.shape[1]

    def halves(a):
        parts = a.reshape(2, half, a.shape[1])
        return pick(parts, core), shift(pick(parts, 1 - core), "core", 1)

    cot_pair = jnp.concatenate(halves(cotangent), 1)
    in_pair = jnp.concatenate(halves(inputs), 1)
    down_pair = jnp.concatenate([w_down, shift(w_down, "core", 1)], 1)
    mine, other = halves(jnp.concatenate([gate_pre, up_pre], 1))
    pre = jnp.where(core == 0, jnp.stack([mine, other]), jnp.stack([other, mine]))

    cot_all = gather_col(cot_pair)
    pre_all = gather_chips(pre.reshape(rows, 2 * ff)).reshape(8 * rows, 2 * ff)
    partial = contract_last(cot_all, down_pair).astype(BF16)
    own = exchange_sum(partial.reshape(8, rows, ff), CHIPS).astype(BF16)
    grad_hidden = gather_chips(own).reshape(8 * rows, ff)

    hidden, gate_grad, up_grad = swiglu_back(pre_all[:, :ff], pre_all[:, ff:], grad_hidden)
    gate_pair = jnp.concatenate([w_gate, shift(w_gate, "core", 1)], 0)
    up_pair = jnp.concatenate([w_up, shift(w_up, "core", 1)], 0)
    back = (contract_last(gate_grad, gate_pair) + contract_last(up_grad, up_pair)).astype(BF16)
    back = exchange_sum_permute(back.reshape(4, 4 * half, 2 * dim), "y").astype(BF16)
    back = exchange_sum_permute(back.reshape(4, half, 2 * dim), "zh").astype(BF16)
    got = shift(back[:, dim:], "core", 1)
    mine = back[:, :dim]
    grad_inputs = jnp.where(
        core == 0, jnp.concatenate([mine, got], 0), jnp.concatenate([got, mine], 0)
    )

    in_all = gather_col(in_pair)
    scale = 1.0 / math.sqrt(16 * rows)
    in_other = shift(in_all[:, dim:], "core", 1)
    cot_other = shift(cot_all[:, dim:], "core", 1)
    in_own = in_all[:, :dim]
    cot_own = cot_all[:, :dim]
    hidden_o = shift(hidden, "core", 1)
    gate_o = shift(gate_grad, "core", 1)
    up_o = shift(up_grad, "core", 1)
    grad_gate = (contract_first(in_own, gate_grad) + contract_first(in_other, gate_o)) * scale
    grad_up = (contract_first(in_own, up_grad) + contract_first(in_other, up_o)) * scale
    grad_down = (contract_first(hidden, cot_own) + contract_first(hidden_o, cot_other)) * scale
    return (grad_inputs, grad_gate, grad_up, grad_down)


def solution(mesh):
    split = Mesh(mesh.devices.reshape(2, 4, 2, 4, 4), ROW + COL)
    in_specs = (
        P(COL, ROW),
        P(COL, ROW),
        P(ROW, COL),
        P(ROW, COL),
        P(ROW, COL),
        P(ROW, COL),
        P(COL, ROW),
    )
    out_specs = (P(COL, ROW), P(ROW, COL), P(ROW, COL), P(COL, ROW))
    return jax.shard_map(
        per_device, mesh=split, in_specs=in_specs, out_specs=out_specs, check_vma=False
    )
```

```python
import math

import jax
import jax.numpy as jnp
from jax import lax
from jax.experimental import pallas as pl
from jax.experimental.pallas import tpu as pltpu
from jax.sharding import Mesh
from jax.sharding import PartitionSpec as P


ROW = ("zl", "x", "core")
COL = ("y", "zh")
CHIPS = ("zl", "x")
BF16 = jnp.bfloat16
F32 = jnp.float32
VMEM = pl.BlockSpec(memory_space=pltpu.VMEM)
SMEM = pl.BlockSpec(memory_space=pltpu.SMEM)
HBM = pl.BlockSpec(memory_space=pltpu.HBM)


def shift(a, axis, by):
    n = lax.axis_size(axis)
    return lax.ppermute(a, axis, [(i, (i + by) % n) for i in range(n)])


def swap(a):
    return shift(a, "core", 1)


def pick(a, i):
    return lax.dynamic_index_in_dim(a, i, 0, False)


def gather(a, axis):
    n = math.prod(lax.axis_size(a) for a in axis)
    return lax.all_to_all(jnp.broadcast_to(a, (n,) + a.shape), axis, 0, 0, tiled=True)


Z_FROM = ((0, 1), (3, 2))
Y_FROM = (0, 1, 3, 2)


def gather_col(a):
    z1 = shift(a, "zh", 1)
    z3 = shift(a, "zh", 3)
    z2 = shift(a, "zh", 2)
    one = jnp.concatenate([a, z1], 0)
    two = jnp.concatenate([z3, z2], 0)
    one_up = shift(one, "y", 1)
    one_down = shift(one, "y", 3)
    two_up = shift(two, "y", 1)
    two_down = shift(two, "y", 3)
    one_far = shift(one_up, "y", 1)
    two_far = shift(two_down, "y", 3)
    return (one, two, one_up, two_up, one_down, two_down, one_far, two_far)


def col_places():
    y, zh = lax.axis_index("y"), lax.axis_index("zh")
    return jnp.stack(
        [((y - by) % 4) * 4 + (zh - bz) % 4 for by in Y_FROM for pair in Z_FROM for bz in pair]
    ).astype(jnp.int32)


def gather_chips(a):
    up = shift(a, "x", 1)
    down = shift(a, "x", -1)
    b = shift(a, "zl", 1)
    far = shift(up, "x", 1)
    b_up = shift(b, "x", 1)
    b_down = shift(b, "x", -1)
    b_far = shift(b_down, "x", -1)
    return (a, up, far, down, b, b_up, b_far, b_down)


def chip_places():
    zl, x = lax.axis_index("zl"), lax.axis_index("x")
    return jnp.stack(
        [((zl + p) % 2) * 4 + (x - by) % 4 for p in range(2) for by in range(4)]
    ).astype(jnp.int32)


def dot_last(left, right):
    return lax.dot_general(left, right, (((1,), (1,)), ((), ())), preferred_element_type=F32)


def dot_first(left, right):
    return lax.dot_general(left, right, (((0,), (0,)), ((), ())), preferred_element_type=F32)


def start(source, target, sem):
    copy = pltpu.make_async_copy(source, target, sem)
    copy.start()
    return copy


def wait(copies):
    for copy in copies:
        copy.wait()


def hidden_kernel(place, *refs):
    pieces, (w_own, w_oth, part, own, oth, cot, w, sums, in_sem, w_sem, out_sem, cot_sem) = refs[:8], refs[8:]
    half, dim = pieces[0].shape[0] // 2, w_own.shape[1]
    loads = [start(w_own, w.at[:, :dim], w_sem.at[0]), start(w_oth, w.at[:, dim:], w_sem.at[1])]
    for n, piece in enumerate(pieces):
        for k in range(2):
            to = pl.ds(pl.multiple_of(place[2 * n + k] * half, half), half)
            loads.append(start(piece.at[k * half : (k + 1) * half], cot.at[to], in_sem.at[2 * n + k]))
    wait(loads)
    stores = [start(cot.at[:, :dim], own, cot_sem.at[0]), start(cot.at[:, dim:], oth, cot_sem.at[1])]
    tile = sums.shape[0] // out_sem.shape[0]

    def step(i, _):
        rows = pl.ds(pl.multiple_of(i * tile, tile), tile)
        sums[rows, :] = dot_last(cot[rows, :], w[...]).astype(BF16)
        pltpu.make_async_copy(sums.at[rows], part.at[rows], out_sem.at[i]).start()
        return 0

    count = out_sem.shape[0]
    lax.fori_loop(0, count, step, 0)
    for i in range(count):
        rows = pl.ds(i * tile, tile)
        pltpu.make_async_copy(sums.at[rows], part.at[rows], out_sem.at[i]).wait()
    wait(stores)


def hidden_partial(pieces, w_own, w_oth):
    tokens = 8 * pieces[0].shape[0]
    ff, dim = w_own.shape
    dma = pltpu.SemaphoreType.DMA
    return pl.pallas_call(
        hidden_kernel,
        out_shape=(
            jax.ShapeDtypeStruct((tokens, ff), BF16),
            jax.ShapeDtypeStruct((tokens, dim), BF16),
            jax.ShapeDtypeStruct((tokens, dim), BF16),
        ),
        in_specs=[SMEM] + [HBM] * 10,
        out_specs=(HBM,) * 3,
        scratch_shapes=[
            pltpu.VMEM((tokens, 2 * dim), BF16),
            pltpu.VMEM((ff, 2 * dim), BF16),
            pltpu.VMEM((tokens, ff), BF16),
            dma((16,)),
            dma((2,)),
            dma((4,)),
            dma((2,)),
        ],
        name="hidden_partial",
    )(col_places(), *pieces, w_own, w_oth)


def place_kernel(place, *refs):
    pieces, (own, oth) = refs[:8], refs[8:]
    half, dim = pieces[0].shape[0] // 2, own.shape[1]
    for n, piece in enumerate(pieces):
        for k in range(2):
            to = pl.ds(pl.multiple_of(place[2 * n + k] * half, half), half)
            own[to, :] = piece[k * half : (k + 1) * half, :dim]
            oth[to, :] = piece[k * half : (k + 1) * half, dim:]


def place_col(pieces, dim):
    out = jax.ShapeDtypeStruct((8 * pieces[0].shape[0], dim), BF16)
    return pl.pallas_call(
        place_kernel,
        out_shape=(out, out),
        in_specs=[SMEM] + [VMEM] * 8,
        out_specs=(VMEM,) * 2,
        name="place_col",
    )(col_places(), *pieces)


def back_kernel(place, mine, *refs):
    pieces, refs = refs[:8], refs[8:]
    grad, weights, (hid_out, gg_out, ug_out), blocks, refs = refs[0], refs[1:5], refs[5:8], refs[8:12], refs[12:]
    pre, gh, w, hid, gg, ug, own, sent, pre_sem, gh_sem, w_sem, out_sem, block_sem = refs
    rows, ff = pieces[0].shape[0], gh.shape[1]
    places = [pl.ds(pl.multiple_of(place[n] * rows, rows), rows) for n in range(8)]
    loads = [
        (start(piece, pre.at[n], pre_sem.at[n]), start(grad.at[to], gh.at[to], gh_sem.at[n]))
        for n, (piece, to) in enumerate(zip(pieces, places))
    ]
    w_loads = [start(a, w.at[n], w_sem.at[n]) for n, a in enumerate(weights)]
    slab, wide = 16, 256
    stores = []
    for n in range(8):
        wait(loads[n])
        base = place[n] * rows

        def step(i, _, n=n, base=base):
            here = pl.ds(pl.multiple_of(i * slab, slab), slab)
            to = pl.ds(pl.multiple_of(base + i * slab, slab), slab)
            for c in range(0, ff, wide):
                at = pl.ds(c, wide)
                gate = pre[n, here, at].astype(F32)
                up = pre[n, here, pl.ds(ff + c, wide)].astype(F32)
                grad = gh[to, at].astype(F32)
                sig = jax.nn.sigmoid(gate)
                act = gate * sig
                hid[to, at] = (act * up).astype(BF16)
                gg[to, at] = (grad * up * sig * (1.0 + gate * (1.0 - sig))).astype(BF16)
                ug[to, at] = (grad * act).astype(BF16)
            return 0

        lax.fori_loop(0, rows // slab, step, 0)
        for k, (a, out) in enumerate(((hid, hid_out), (gg, gg_out), (ug, ug_out))):
            stores.append(start(a.at[places[n]], out.at[places[n]], out_sem.at[n, k]))
    wait(w_loads)
    tile, dim, cut = own.shape[0], w.shape[1], 256
    for s in (2, 1, 3, 0):
        at = pl.ds(pl.multiple_of(((mine[0] + s) % 4) * tile, tile), tile)
        block = own if s == 0 else sent.at[s - 1]

        def part(j, _, at=at, block=block):
            for side in range(2):
                take = pl.ds(pl.multiple_of(j * cut, cut), cut)
                to = pl.ds(pl.multiple_of(side * dim + j * cut, cut), cut)
                acc = dot_last(gg[at, :], w[side, take, :]) + dot_last(ug[at, :], w[2 + side, take, :])
                block[:, to] = acc.astype(block.dtype)
            return 0

        lax.fori_loop(0, dim // cut, part, 0)
        stores.append(start(block, blocks[s], block_sem.at[s]))
    wait(stores)


def back_partial(pieces, grad_hidden, weights):
    tokens, ff = grad_hidden.shape
    full = jax.ShapeDtypeStruct((tokens, ff), BF16)
    tile, dim = tokens // 4, weights[0].shape[0]
    dma = pltpu.SemaphoreType.DMA
    return pl.pallas_call(
        back_kernel,
        out_shape=(full,) * 3
        + tuple(jax.ShapeDtypeStruct((tile, 2 * dim), F32 if s == 0 else BF16) for s in range(4)),
        in_specs=[SMEM] * 2 + [HBM] * 13,
        out_specs=(HBM,) * 7,
        scratch_shapes=[
            pltpu.VMEM((8, tokens // 8, 2 * ff), BF16),
            pltpu.VMEM((tokens, ff), BF16),
            pltpu.VMEM((4, dim, ff), BF16),
            pltpu.VMEM((tokens, ff), BF16),
            pltpu.VMEM((tokens, ff), BF16),
            pltpu.VMEM((tokens, ff), BF16),
            pltpu.VMEM((tile, 2 * dim), F32),
            pltpu.VMEM((3, tile, 2 * dim), BF16),
            dma((8,)),
            dma((8,)),
            dma((4,)),
            dma((8, 3)),
            dma((4,)),
        ],
        name="back_partial",
    )(chip_places(), lax.axis_index("y").astype(jnp.int32)[None], *pieces, grad_hidden, *weights)


def sum_kernel(mine, b0, r1, r2, r3, s0, s1, s2, s3):
    tile = s0.shape[0]
    for s, out in ((1, s1), (3, s3), (2, s2), (0, s0)):
        at = pl.ds(pl.multiple_of(((mine[0] + s) % 4) * tile, tile), tile)
        total = b0[at, :] + r1[at, :].astype(F32) + r2[at, :].astype(F32) + r3[at, :].astype(F32)
        out[...] = total.astype(out.dtype)


def sum_blocks(blocks):
    rows, n = blocks[0].shape
    return pl.pallas_call(
        sum_kernel,
        out_shape=tuple(
            jax.ShapeDtypeStruct((rows // 4, n), F32 if s == 0 else BF16) for s in range(4)
        ),
        in_specs=[SMEM] + [VMEM] * 4,
        out_specs=(VMEM,) * 4,
        name="sum_blocks",
    )(lax.axis_index("zh").astype(jnp.int32)[None], *blocks)


def send_back(blocks, axis):
    b0, b1, b2, b3 = blocks
    r1 = shift(b1, axis, 1)
    r3 = shift(b3, axis, 3)
    r2 = shift(b2, axis, 2)
    return b0, r1, r2, r3


def layer(inputs, cotangent, gate_pre, up_pre, w_gate, w_up, w_down):
    core = lax.axis_index("core")
    rows = inputs.shape[0]
    half = rows // 2
    dim = inputs.shape[1]
    ff = gate_pre.shape[1]

    def halves(a):
        parts = a.reshape(2, half, a.shape[1])
        return pick(parts, core), swap(pick(parts, 1 - core))

    cot_pair = jnp.concatenate(halves(cotangent), 1)
    mine, other = halves(jnp.concatenate([gate_pre, up_pre], 1))
    pre = jnp.where(core == 0, jnp.stack([mine, other]), jnp.stack([other, mine]))
    down_other = swap(w_down)
    in_pair = jnp.concatenate(halves(inputs), 1)

    cot_pieces = gather_col(cot_pair)
    pre_pieces = gather_chips(pre.reshape(rows, 2 * ff))
    partial, cot_own, cot_send = hidden_partial(cot_pieces, w_down, down_other)
    got = lax.all_to_all(partial.reshape(8, rows, ff), CHIPS, 0, 0, tiled=True)
    own = got.astype(F32).sum(0).astype(BF16)
    grad_hidden = gather(own, CHIPS).reshape(8 * rows, ff)

    weights = (w_gate, swap(w_gate), w_up, swap(w_up))
    hidden, gate_grad, up_grad, *blocks = back_partial(pre_pieces, grad_hidden, weights)
    blocks = sum_blocks(send_back(blocks, "y"))
    back = sum(b.astype(F32) for b in send_back(blocks, "zh")).astype(BF16)
    got = swap(back[:, dim:])
    mine = back[:, :dim]
    grad_inputs = jnp.where(
        core == 0, jnp.concatenate([mine, got], 0), jnp.concatenate([got, mine], 0)
    )

    in_own, in_send = place_col(gather_col(in_pair), dim)
    scale = 1.0 / math.sqrt(16 * rows)
    in_oth = swap(in_send)
    cot_oth = swap(cot_send)
    hidden_o = swap(hidden)
    gate_o = swap(gate_grad)
    up_o = swap(up_grad)
    grad_down = (dot_first(hidden, cot_own) + dot_first(hidden_o, cot_oth)) * scale
    grad_gate = (dot_first(in_own, gate_grad) + dot_first(in_oth, gate_o)) * scale
    grad_up = (dot_first(in_own, up_grad) + dot_first(in_oth, up_o)) * scale
    return (grad_inputs, grad_gate, grad_up, grad_down)


def solution(mesh):
    split = Mesh(mesh.devices.reshape(2, 4, 2, 4, 4), ROW + COL)
    in_specs = (
        P(COL, ROW),
        P(COL, ROW),
        P(ROW, COL),
        P(ROW, COL),
        P(ROW, COL),
        P(ROW, COL),
        P(COL, ROW),
    )
    out_specs = (P(COL, ROW), P(ROW, COL), P(ROW, COL), P(COL, ROW))
    return jax.shard_map(layer, mesh=split, in_specs=in_specs, out_specs=out_specs, check_vma=False)
```
